32 devices in a mesh: chan: 8 (over z, y), bins: 4 (over x, core).
Axes of the slice: x: 2, y: 2, z: 4, core: 2. Of those that a mesh axis runs over, the one named last changes fastest.
Arguments:
- effects: bfloat16 [64, 8192, 256], P('chan', 'bins'), may hold values from -0.19921875 to 0.19921875
- nominal: float32 [64, 8192], P('chan', 'bins'), may hold values from 0.2 to 5
- observed: int32 [64, 8192], P('chan', 'bins'), may hold values from 0 to 7
- mc_variance: float32 [64, 8192], P('chan', 'bins'), may hold values from 0.002 to 0.5
- theta: float32 [8192], replicated, may hold values from -4 to 4
- nuisance_index: int32 [64, 256], replicated, may hold values from 0 to 8191, as said below
- bin_counts: int32 [64], P('chan'), may hold values from 1 to 8192, 262144 in all
- tile_owner: int32 [256], replicated, may hold values from 0 to 255, each once
Outputs:
- hessian_tiles: float32 [256, 512, 512], P(('chan', 'bins'))
- gradient: float32 [8192], P(('chan', 'bins'))
The draws below stay inside these ranges and needn't reach their ends.
Inputs may be any that keep to these rules, and one draw needn't show every extreme that they name: `nuisance_index`: each channel's list is 2 runs of 128 consecutive nuisances, each run starting at a multiple of 128, the runs distinct and in increasing order. Bins at positions bin_counts[c] and beyond of channel c carry no data. `tile_owner`: every tile number appears exactly once.
All inputs are finite; a program needn't handle non-finite values. No bound on the sum of `bin_counts` on one device may be relied on, other than what follows from the above.
Results may differ from the reference program's by a relative error of at most 0.0029.
Values sent between devices are 32-bit elements; how exact they have to be, the bound alone decides.
A program may use at most 128 MiB of HBM per device.

```python
import math
import jax
import jax.numpy as jnp
import numpy as np
from jax import lax

NU = 8192
K = 256
GW = 128
TILE = 512
CH = 64
BC = 8192
NTS = 16
NT = 256


def draw_nuisance_index(key, part):
    group_count = NU // GW
    group_parts = K // GW
    channel_keys = jax.random.split(jax.random.fold_in(key, 17), CH)

    def one_channel(channel_key):
        shuffled = jax.random.permutation(channel_key, group_count)
        picked = jnp.sort(shuffled[:group_parts])
        return (picked[:, None] * GW + jnp.arange(GW)[None, :]).reshape(-1)
    return jax.vmap(one_channel)(channel_keys).astype(jnp.int32)


def with_ends(values, rng, least, top_value):
    dims = values.shape
    place = [jax.random.randint(jax.random.fold_in(rng, axis), (), 0, dims[axis]) for axis in range(len(dims))]
    values = values.at[tuple(place)].set(least)
    longest = dims.index(max(dims))
    place[longest] = (place[longest] + 1) % dims[longest]
    return values.at[tuple(place)].set(top_value)


def levels(stream_key, extent, shards, least, largest):
    factor_of = 1.0
    for position, shards_of in shards:
        steps = jax.random.uniform(jax.random.fold_in(jax.random.fold_in(stream_key, 6), position), (shards_of,), jnp.float32, least / len(shards), largest / len(shards))
        factor_of = factor_of * jnp.repeat(jnp.exp(steps), extent[position] // shards_of).reshape((-1,) + (1,) * (len(extent) - 1 - position))
    return factor_of


def split_up(amount, total, most, slope):
    loads = [(1 << 20) // math.isqrt(grade ** slope) + 1 for grade in range(2, amount + 1)]
    surplus, given = total - most - (amount - 1), [1] * (amount - 1)
    while surplus > 0:
        candidates = [i for i in range(amount - 1) if given[i] < most]
        whole, remaining = sum([loads[i] for i in candidates]), surplus
        for i in candidates:
            extra = min(most - given[i], max(1, remaining * loads[i] // whole), surplus)
            given[i] = given[i] + extra
            surplus = surplus - extra
    return np.array([most] + given)


def ragged_sizes(rng, number_of, total, limit, lean):
    if number_of == 2:
        one = jax.random.randint(rng, (), max(1, total - limit), min(limit, total - 1) + 1)
        return jnp.stack([one, total - one])
    tallies = jnp.asarray(split_up(number_of, total, limit, lean), jnp.int32)
    pairs = (number_of - 1) // 2
    giver, receiver = tallies[1:1 + 2 * pairs:2], tallies[2:2 + 2 * pairs:2]
    margin = jnp.minimum(giver - 1, limit - receiver)
    moved = jax.random.randint(jax.random.fold_in(rng, 1), (pairs,), 0, 1 << 20) % (margin + 1)
    tallies = tallies.at[1:1 + 2 * pairs:2].set(giver - moved).at[2:2 + 2 * pairs:2].set(receiver + moved)
    return tallies[jax.random.permutation(jax.random.fold_in(rng, 2), number_of)]


def gaussian(own_key, extent, spread, most, cuts=(), kind=jnp.bfloat16):
    level = levels(own_key, extent, cuts, -0.22, 0.18) if cuts else 1.0
    result = jax.random.normal(own_key, extent, jnp.float32) * spread * level
    return jnp.minimum(jnp.maximum(result, -most), most).astype(kind)


def setup_inputs(seed: int = 0) -> dict:
    arg_keys = jax.random.split(jax.random.key(seed), 9)
    return {
        "effects": gaussian(arg_keys[0], (CH, BC, K), 0.04, 0.19921875, ((0, 8), (1, 4))),
        "nominal": jnp.clip(jnp.exp(math.log(5.0) - 3.218876 * jax.random.uniform(arg_keys[1], (CH, BC), jnp.float32) ** levels(arg_keys[1], (CH, BC), ((0, 8), (1, 4)), -0.2, 0.2)), 0.2, 5.0),
        "observed": with_ends(jax.random.randint(arg_keys[2], (CH, BC), 0, 8), jax.random.fold_in(arg_keys[2], 1), 0, 7).astype(jnp.int32),
        "mc_variance": jnp.clip(jnp.exp(math.log(0.5) - 5.521461 * jax.random.uniform(arg_keys[3], (CH, BC), jnp.float32) ** levels(arg_keys[3], (CH, BC), ((0, 8), (1, 4)), -0.2, 0.2)), 0.002, 0.5),
        "theta": gaussian(arg_keys[4], (NU,), 1.0, 4.0, (), jnp.float32),
        "nuisance_index": draw_nuisance_index(jax.random.fold_in(arg_keys[8], 71), 0),
        "bin_counts": ragged_sizes(arg_keys[6], CH, CH * BC // 2, BC, 2).astype(jnp.int32),
        "tile_owner": jax.random.permutation(arg_keys[7], NT).astype(jnp.int32),
    }


def reference(effects, nominal, observed, mc_variance, theta, nuisance_index, bin_counts, tile_owner):
    positions = jnp.arange(BC, dtype=jnp.int32)

    def channel_step(carry, inputs):
        hessian, gradient = carry
        matrix, nominal_row, observed_row, variance_row, indices, used = inputs
        chosen = theta[indices].astype(jnp.bfloat16)
        exponent = jnp.dot(matrix, chosen, preferred_element_type=jnp.float32)
        expected = nominal_row * jnp.exp(exponent)
        denominator = 1.0 + expected * variance_row
        live = positions < used
        residual = jnp.where(live, (expected - observed_row) / denominator, 0.0)
        weight = jnp.where(live, expected / denominator, 0.0)
        scaled = (jnp.sqrt(weight)[:, None] * matrix).astype(jnp.bfloat16)
        block = jnp.dot(scaled.T, scaled, preferred_element_type=jnp.float32)
        gradient_part = jnp.dot(residual.astype(jnp.bfloat16), matrix, preferred_element_type=jnp.float32)
        hessian = hessian.at[indices[:, None], indices[None, :]].add(block)
        gradient = gradient.at[indices].add(gradient_part)
        return ((hessian, gradient), None)
    initial = (jnp.zeros((NU, NU), jnp.float32), jnp.zeros((NU,), jnp.float32))
    totals, ignored = lax.scan(channel_step, initial, (effects, nominal, observed, mc_variance, nuisance_index, bin_counts))
    hessian = totals[0] + jnp.eye(NU, dtype=jnp.float32)
    tiles = hessian.reshape(NTS, TILE, NTS, TILE).transpose(0, 2, 1, 3).reshape(NT, TILE, TILE)
    return (tiles[tile_owner], totals[1] + theta)
```

```python
import functools

import jax
import jax.numpy as jnp
from jax import lax
from jax.experimental import pallas as pl
from jax.experimental.pallas import tpu as pltpu
from jax.sharding import PartitionSpec as P

GW = 128
TILE = 512
EXTRA = 8


def channel_payload(eff, chosen, nominal, observed, variance, live):
    eff_t = eff.T
    exponent = jnp.dot(chosen, eff_t, preferred_element_type=jnp.float32)[0:8]
    expected = nominal * jnp.exp(exponent)
    denominator = 1.0 + expected * variance
    residual = jnp.where(live, (expected - observed) / denominator, 0.0)
    weight = jnp.where(live, expected / denominator, 0.0)
    weighted = (eff_t.astype(jnp.float32) * weight[0:1]).astype(jnp.bfloat16)
    residual_rows = jnp.concatenate([residual, residual], axis=0).astype(jnp.bfloat16)
    left = jnp.concatenate([weighted, residual_rows], axis=0)
    full = jnp.dot(left, eff, preferred_element_type=jnp.float32)
    first, off, second = full[:GW, :GW], full[:GW, GW:], full[GW : 2 * GW, GW:]
    row = lax.broadcasted_iota(jnp.int32, (GW, GW), 0)
    col = lax.broadcasted_iota(jnp.int32, (GW, GW), 1)
    packed = jnp.where(row <= col, first, second)
    second_diag = jnp.sum(jnp.where(row == col, second, 0.0), axis=0, keepdims=True)
    grad0 = full[2 * GW : 2 * GW + 8, :GW]
    grad1 = full[2 * GW : 2 * GW + 8, GW:]
    which = lax.broadcasted_iota(jnp.int32, (EXTRA, GW), 0)
    extra = jnp.where(
        which == 0, grad0, jnp.where(which == 1, grad1, jnp.broadcast_to(second_diag, (EXTRA, GW)))
    )
    return packed, off, extra


def curvature_kernel(groups_ref, counts_ref, eff_ref, nom_ref, obs_ref, var_ref, theta_ref, out_ref):
    chan = lax.axis_index("chan")
    bins = lax.axis_index("bins")
    c = pl.program_id(0)
    size = eff_ref.shape[1]
    base = chan * pl.num_programs(0) + c
    g0, g1 = groups_ref[base, 0], groups_ref[base, 1]
    chosen = jnp.concatenate([theta_ref[g0], theta_ref[g1]], axis=1).astype(jnp.bfloat16)
    chosen = jnp.broadcast_to(chosen, (16, 2 * GW))
    nominal, observed, variance = nom_ref[c], obs_ref[c].astype(jnp.float32), var_ref[c]
    position = bins * size + lax.broadcasted_iota(jnp.int32, (8, size), 1)
    packed, off, extra = channel_payload(
        eff_ref[0], chosen, nominal, observed, variance, position < counts_ref[c]
    )
    out_ref[0, :GW] = packed
    out_ref[0, GW : 2 * GW] = off
    out_ref[0, 2 * GW :] = extra


def curvature(effects, nominal, observed, variance, theta, groups, counts):
    chans, size, width = effects.shape
    rows = 2 * GW + EXTRA
    whole = lambda *shape: pl.BlockSpec(shape, lambda c, *_: (0,) * len(shape))
    return pl.pallas_call(
        curvature_kernel,
        grid_spec=pltpu.PrefetchScalarGridSpec(
            num_scalar_prefetch=2,
            grid=(chans,),
            in_specs=[
                pl.BlockSpec((1, size, width), lambda c, *_: (c, 0, 0)),
                whole(chans, 1, size),
                whole(chans, 1, size),
                whole(chans, 1, size),
                whole(theta.shape[0] // GW, 1, GW),
            ],
            out_specs=pl.BlockSpec((1, rows, GW), lambda c, *_: (c, 0, 0)),
        ),
        out_shape=jax.ShapeDtypeStruct((chans, rows, GW), jnp.float32),
        compiler_params=pltpu.CompilerParams(vmem_limit_bytes=40 * 2**20),
        name="curvature",
    )(
        groups,
        counts,
        effects,
        nominal.reshape(chans, 1, size),
        observed.reshape(chans, 1, size),
        variance.reshape(chans, 1, size),
        theta.reshape(-1, 1, GW),
    )


def place_kernel(
    groups_ref, owner_ref, payload_ref, theta_ref, tiles_ref, grad_ref,
    held, grads, lookup, entries, counts, waited, held_sem, grad_sem,
):
    step = pl.program_id(0)
    slots = pl.num_programs(0)
    device = lax.axis_index("chan") * lax.axis_size("bins") + lax.axis_index("bins")
    chans = payload_ref.shape[0]
    per_tile = TILE // GW
    total_groups = theta_ref.shape[0]
    side = total_groups // per_tile
    room = entries.shape[0] // counts.shape[0]
    start = device * slots

    def copy_of(c):
        return pltpu.make_async_copy(
            payload_ref.at[c, pl.ds(0, 2 * GW + EXTRA)], held.at[c], held_sem.at[c]
        )

    grad_copy = pltpu.make_async_copy(
        payload_ref.at[:, pl.ds(2 * GW, EXTRA)], grads, grad_sem.at[0]
    )

    @pl.when(step == 0)
    def _():
        grad_copy.start()

        def clear(i, _):
            for j in range(16):
                lookup[i * 16 + j] = -1
            return 0

        lax.fori_loop(0, side * side // 16, clear, 0)
        for s in range(counts.shape[0]):
            counts[s] = 0
            lookup[owner_ref[start + s]] = s

        def visit(c, _):
            a, b = groups_ref[c, 0], groups_ref[c, 1]
            ta, tb = a // per_tile, b // per_tile
            ra, rb = a % per_tile, b % per_tile
            hits = []
            for kind, (tr, tc, rr, rc) in enumerate(
                ((ta, ta, ra, ra), (tb, tb, rb, rb), (ta, tb, ra, rb), (tb, ta, rb, ra))
            ):
                slot = lookup[tr * side + tc]
                hits.append(slot)

                @pl.when(slot >= 0)
                def _(slot=slot, kind=kind, rr=rr, rc=rc):
                    n = counts[slot]
                    entries[slot * room + n] = ((c * per_tile + rr) * per_tile + rc) * 4 + kind
                    counts[slot] = n + 1

            used = jnp.maximum(jnp.maximum(hits[0], hits[1]), jnp.maximum(hits[2], hits[3])) >= 0
            waited[c] = jnp.where(used, 0, 1)

            @pl.when(used)
            def _():
                copy_of(c).start()

            return 0

        lax.fori_loop(0, chans, visit, 0)

    tile = owner_ref[start + step]

    tiles_ref[...] = jnp.zeros_like(tiles_ref)
    eye = (
        lax.broadcasted_iota(jnp.int32, (GW, GW), 0) == lax.broadcasted_iota(jnp.int32, (GW, GW), 1)
    ).astype(jnp.float32)

    @pl.when(tile // side == tile % side)
    def _():
        for r in range(per_tile):
            tiles_ref[0, r * GW : (r + 1) * GW, r * GW : (r + 1) * GW] = eye

    row = lax.broadcasted_iota(jnp.int32, (GW, GW), 0)
    col = lax.broadcasted_iota(jnp.int32, (GW, GW), 1)

    def accumulate(i, _):
        code = entries[step * room + i]
        kind = code % 4
        rc = code // 4 % per_tile
        rr = code // (4 * per_tile) % per_tile
        c = code // (4 * per_tile * per_tile)

        @pl.when(waited[c] == 0)
        def _():
            copy_of(c).wait()
            waited[c] = 1

        at = (
            0,
            pl.ds(pl.multiple_of(rr * GW, GW), GW),
            pl.ds(pl.multiple_of(rc * GW, GW), GW),
        )

        @pl.when(kind == 0)
        def _():
            upper = jnp.where(row <= col, held[c, :GW], 0.0)
            tiles_ref[at] += upper + jnp.where(row > col, upper.T, 0.0)

        @pl.when(kind == 1)
        def _():
            lower = jnp.where(row > col, held[c, :GW], 0.0)
            diag = jnp.where(row == col, held[c, 2 * GW + 2 : 2 * GW + 3], 0.0)
            tiles_ref[at] += lower + lower.T + diag

        @pl.when(kind == 2)
        def _():
            tiles_ref[at] += held[c, GW : 2 * GW]

        @pl.when(kind == 3)
        def _():
            tiles_ref[at] += held[c, GW : 2 * GW].T

        return 0

    lax.fori_loop(0, counts[step], accumulate, 0)

    @pl.when(step == slots - 1)
    def _():
        grad_copy.wait()
        mine = grad_ref.shape[0]
        first = device * total_groups // (lax.axis_size("chan") * lax.axis_size("bins"))
        for m in range(mine):
            grad_ref[m] = theta_ref[first + m]

        def add(c, _):
            for r in range(2):
                m = groups_ref[c, r] - first

                @pl.when(jnp.logical_and(m >= 0, m < mine))
                def _(m=m, r=r):
                    grad_ref[m] += grads[c, r : r + 1]

            return 0

        lax.fori_loop(0, chans, add, 0)


def place(payload, theta, groups, tile_owner, slots, mine):
    chans, rows = payload.shape[:2]
    return pl.pallas_call(
        place_kernel,
        grid_spec=pltpu.PrefetchScalarGridSpec(
            num_scalar_prefetch=2,
            grid=(slots,),
            in_specs=[
                pl.BlockSpec(memory_space=pl.ANY),
                pl.BlockSpec((theta.shape[0] // GW, 1, GW), lambda s, *_: (0, 0, 0)),
            ],
            out_specs=[
                pl.BlockSpec((1, TILE, TILE), lambda s, *_: (s, 0, 0)),
                pl.BlockSpec((mine, 1, GW), lambda s, *_: (0, 0, 0)),
            ],
            scratch_shapes=[
                pltpu.VMEM((chans, rows, GW), jnp.float32),
                pltpu.VMEM((chans, EXTRA, GW), jnp.float32),
                pltpu.SMEM((tile_owner.shape[0],), jnp.int32),
                pltpu.SMEM((slots * chans * 4,), jnp.int32),
                pltpu.SMEM((slots,), jnp.int32),
                pltpu.SMEM((chans,), jnp.int32),
                pltpu.SemaphoreType.DMA((chans,)),
                pltpu.SemaphoreType.DMA((1,)),
            ],
        ),
        out_shape=[
            jax.ShapeDtypeStruct((slots, TILE, TILE), jnp.float32),
            jax.ShapeDtypeStruct((mine, 1, GW), jnp.float32),
        ],
        compiler_params=pltpu.CompilerParams(vmem_limit_bytes=50 * 2**20),
        name="place",
    )(groups, tile_owner, payload, theta.reshape(-1, 1, GW))


def local(effects, nominal, observed, mc_variance, theta, nuisance_index, bin_counts, tile_owner):
    devices = lax.axis_size("chan") * lax.axis_size("bins")
    device = lax.axis_index("chan") * lax.axis_size("bins") + lax.axis_index("bins")
    total_nu = theta.shape[0]
    slice_len = total_nu // devices
    groups = nuisance_index[:, ::GW] // GW
    parts = curvature(effects, nominal, observed, mc_variance, theta, groups, bin_counts)
    summed = lax.psum_scatter(parts, "bins", scatter_dimension=0, tiled=True)
    payload = lax.all_gather(summed, ("chan", "bins"), axis=0, tiled=True)
    tiles, grad = place(
        payload, theta, groups, tile_owner, tile_owner.shape[0] // devices, max(1, slice_len // GW)
    )
    gradient = grad.reshape(-1)
    if slice_len < GW:
        gradient = lax.dynamic_slice_in_dim(gradient, device * slice_len % GW, slice_len, 0)
    return (tiles, gradient)


def solution(mesh):
    return jax.shard_map(
        local,
        mesh=mesh,
        in_specs=(
            P("chan", "bins", None),
            P("chan", "bins"),
            P("chan", "bins"),
            P("chan", "bins"),
            P(),
            P(),
            P("chan"),
            P(),
        ),
        out_specs=(P(("chan", "bins"), None, None), P(("chan", "bins"))),
        check_vma=False,
    )
```

```python
import functools

import jax
import jax.numpy as jnp
from jax import lax
from jax.experimental import pallas as pl
from jax.experimental.pallas import tpu as pltpu
from jax.sharding import PartitionSpec as P

GW = 128
TILE = 512
EXTRA = 8


def channel_payload(eff, chosen, nominal, observed, variance, live):
    eff_t = eff.T
    exponent = jnp.dot(chosen, eff_t, preferred_element_type=jnp.float32)[0:8]
    expected = nominal * jnp.exp(exponent)
    denominator = 1.0 + expected * variance
    residual = jnp.where(live, (expected - observed) / denominator, 0.0)
    weight = jnp.where(live, expected / denominator, 0.0)
    weighted = (eff_t.astype(jnp.float32) * weight[0:1]).astype(jnp.bfloat16)
    residual_rows = jnp.concatenate([residual, residual], axis=0).astype(jnp.bfloat16)
    left = jnp.concatenate([weighted, residual_rows], axis=0)
    full = jnp.dot(left, eff, preferred_element_type=jnp.float32)
    first, off, second = full[:GW, :GW], full[:GW, GW:], full[GW : 2 * GW, GW:]
    row = lax.broadcasted_iota(jnp.int32, (GW, GW), 0)
    col = lax.broadcasted_iota(jnp.int32, (GW, GW), 1)
    packed = jnp.where(row <= col, first, second)
    second_diag = jnp.sum(jnp.where(row == col, second, 0.0), axis=0, keepdims=True)
    grad0 = full[2 * GW : 2 * GW + 8, :GW]
    grad1 = full[2 * GW : 2 * GW + 8, GW:]
    which = lax.broadcasted_iota(jnp.int32, (EXTRA, GW), 0)
    extra = jnp.where(
        which == 0, grad0, jnp.where(which == 1, grad1, jnp.broadcast_to(second_diag, (EXTRA, GW)))
    )
    return packed, off, extra


def curvature_kernel(groups_ref, counts_ref, eff_ref, nom_ref, obs_ref, var_ref, theta_ref, out_ref):
    chan = lax.axis_index("chan")
    bins = lax.axis_index("bins")
    c = pl.program_id(0)
    size = eff_ref.shape[1]
    base = chan * pl.num_programs(0) + c
    g0, g1 = groups_ref[base, 0], groups_ref[base, 1]
    chosen = jnp.concatenate([theta_ref[g0], theta_ref[g1]], axis=1).astype(jnp.bfloat16)
    chosen = jnp.broadcast_to(chosen, (16, 2 * GW))
    line = pl.ds(c, 1)
    nominal, observed, variance = nom_ref[line], obs_ref[line].astype(jnp.float32), var_ref[line]
    position = bins * size + lax.broadcasted_iota(jnp.int32, (8, size), 1)
    packed, off, extra = channel_payload(
        eff_ref[0], chosen, nominal, observed, variance, position < counts_ref[c]
    )
    out_ref[0, :GW] = packed
    out_ref[0, GW : 2 * GW] = off
    out_ref[0, 2 * GW :] = extra


def curvature(effects, nominal, observed, variance, theta, groups, counts):
    chans, size, width = effects.shape
    rows = 2 * GW + EXTRA
    whole = lambda *shape: pl.BlockSpec(shape, lambda c, *_: (0,) * len(shape))
    return pl.pallas_call(
        curvature_kernel,
        grid_spec=pltpu.PrefetchScalarGridSpec(
            num_scalar_prefetch=2,
            grid=(chans,),
            in_specs=[
                pl.BlockSpec((1, size, width), lambda c, *_: (c, 0, 0)),
                whole(chans, size),
                whole(chans, size),
                whole(chans, size),
                whole(theta.shape[0] // GW, 1, GW),
            ],
            out_specs=pl.BlockSpec((1, rows, GW), lambda c, *_: (c, 0, 0)),
        ),
        out_shape=jax.ShapeDtypeStruct((chans, rows, GW), jnp.float32),
        compiler_params=pltpu.CompilerParams(vmem_limit_bytes=58 * 2**20),
        name="curvature",
    )(
        groups,
        counts,
        effects,
        nominal,
        observed,
        variance,
        theta.reshape(-1, 1, GW),
    )


def place_kernel(
    groups_ref, owner_ref, payload_ref, theta_ref, tiles_ref, grad_ref,
    held, grads, lookup, entries, counts, waited, held_sem, grad_sem,
):
    step = pl.program_id(0)
    slots = pl.num_programs(0)
    device = lax.axis_index("chan") * lax.axis_size("bins") + lax.axis_index("bins")
    chans = payload_ref.shape[0]
    per_tile = TILE // GW
    total_groups = theta_ref.shape[0]
    side = total_groups // per_tile
    room = entries.shape[0] // counts.shape[0]
    start = device * slots

    def copy_of(c):
        return pltpu.make_async_copy(
            payload_ref.at[c, pl.ds(0, 2 * GW + EXTRA)], held.at[c], held_sem.at[c]
        )

    grad_copy = pltpu.make_async_copy(
        payload_ref.at[:, pl.ds(2 * GW, EXTRA)], grads, grad_sem.at[0]
    )

    @pl.when(step == 0)
    def _():
        grad_copy.start()

        def clear(i, _):
            for j in range(16):
                lookup[i * 16 + j] = -1
            return 0

        lax.fori_loop(0, side * side // 16, clear, 0)
        for s in range(counts.shape[0]):
            counts[s] = 0
            lookup[owner_ref[start + s]] = s

        def visit(c, _):
            a, b = groups_ref[c, 0], groups_ref[c, 1]
            ta, tb = a // per_tile, b // per_tile
            ra, rb = a % per_tile, b % per_tile
            hits = []
            for kind, (tr, tc, rr, rc) in enumerate(
                ((ta, ta, ra, ra), (tb, tb, rb, rb), (ta, tb, ra, rb), (tb, ta, rb, ra))
            ):
                slot = lookup[tr * side + tc]
                hits.append(slot)

                @pl.when(slot >= 0)
                def _(slot=slot, kind=kind, rr=rr, rc=rc):
                    n = counts[slot]
                    entries[slot * room + n] = ((c * per_tile + rr) * per_tile + rc) * 4 + kind
                    counts[slot] = n + 1

            used = jnp.maximum(jnp.maximum(hits[0], hits[1]), jnp.maximum(hits[2], hits[3])) >= 0
            waited[c] = jnp.where(used, 0, 1)

            @pl.when(used)
            def _():
                copy_of(c).start()

            return 0

        lax.fori_loop(0, chans, visit, 0)

    tile = owner_ref[start + step]

    tiles_ref[...] = jnp.zeros_like(tiles_ref)
    eye = (
        lax.broadcasted_iota(jnp.int32, (GW, GW), 0) == lax.broadcasted_iota(jnp.int32, (GW, GW), 1)
    ).astype(jnp.float32)

    @pl.when(tile // side == tile % side)
    def _():
        for r in range(per_tile):
            tiles_ref[0, r * GW : (r + 1) * GW, r * GW : (r + 1) * GW] = eye

    row = lax.broadcasted_iota(jnp.int32, (GW, GW), 0)
    col = lax.broadcasted_iota(jnp.int32, (GW, GW), 1)

    def accumulate(i, _):
        code = entries[step * room + i]
        kind = code % 4
        rc = code // 4 % per_tile
        rr = code // (4 * per_tile) % per_tile
        c = code // (4 * per_tile * per_tile)

        @pl.when(waited[c] == 0)
        def _():
            copy_of(c).wait()
            waited[c] = 1

        at = (
            0,
            pl.ds(pl.multiple_of(rr * GW, GW), GW),
            pl.ds(pl.multiple_of(rc * GW, GW), GW),
        )

        @pl.when(kind == 0)
        def _():
            upper = jnp.where(row <= col, held[c, :GW], 0.0)
            tiles_ref[at] += upper + jnp.where(row > col, upper.T, 0.0)

        @pl.when(kind == 1)
        def _():
            lower = jnp.where(row > col, held[c, :GW], 0.0)
            diag = jnp.where(row == col, held[c, 2 * GW + 2 : 2 * GW + 3], 0.0)
            tiles_ref[at] += lower + lower.T + diag

        @pl.when(kind == 2)
        def _():
            tiles_ref[at] += held[c, GW : 2 * GW]

        @pl.when(kind == 3)
        def _():
            tiles_ref[at] += held[c, GW : 2 * GW].T

        return 0

    lax.fori_loop(0, counts[step], accumulate, 0)

    @pl.when(step == slots - 1)
    def _():
        grad_copy.wait()
        mine = grad_ref.shape[0]
        first = device * total_groups // (lax.axis_size("chan") * lax.axis_size("bins"))
        for m in range(mine):
            grad_ref[m] = theta_ref[first + m]

        def add(c, _):
            for r in range(2):
                m = groups_ref[c, r] - first

                @pl.when(jnp.logical_and(m >= 0, m < mine))
                def _(m=m, r=r):
                    grad_ref[m] += grads[c, r : r + 1]

            return 0

        lax.fori_loop(0, chans, add, 0)


def place(payload, theta, groups, tile_owner, slots, mine):
    chans, rows = payload.shape[:2]
    return pl.pallas_call(
        place_kernel,
        grid_spec=pltpu.PrefetchScalarGridSpec(
            num_scalar_prefetch=2,
            grid=(slots,),
            in_specs=[
                pl.BlockSpec(memory_space=pl.ANY),
                pl.BlockSpec((theta.shape[0] // GW, 1, GW), lambda s, *_: (0, 0, 0)),
            ],
            out_specs=[
                pl.BlockSpec((1, TILE, TILE), lambda s, *_: (s, 0, 0)),
                pl.BlockSpec((mine, 1, GW), lambda s, *_: (0, 0, 0)),
            ],
            scratch_shapes=[
                pltpu.VMEM((chans, rows, GW), jnp.float32),
                pltpu.VMEM((chans, EXTRA, GW), jnp.float32),
                pltpu.SMEM((tile_owner.shape[0],), jnp.int32),
                pltpu.SMEM((slots * chans * 4,), jnp.int32),
                pltpu.SMEM((slots,), jnp.int32),
                pltpu.SMEM((chans,), jnp.int32),
                pltpu.SemaphoreType.DMA((chans,)),
                pltpu.SemaphoreType.DMA((1,)),
            ],
        ),
        out_shape=[
            jax.ShapeDtypeStruct((slots, TILE, TILE), jnp.float32),
            jax.ShapeDtypeStruct((mine, 1, GW), jnp.float32),
        ],
        compiler_params=pltpu.CompilerParams(
            vmem_limit_bytes=4 * chans * (rows + EXTRA) * GW + 8 * 2**20
        ),
        name="place",
    )(groups, tile_owner, payload, theta.reshape(-1, 1, GW))


COLORS = ((0, 104, "zxy"), (104, 104, "zyx"), (208, 56, "xyz"))
DEEP = 4


def exchange_kernel(ydim, parts_ref, out_ref, swap, cross, total, swap_recv, cross_recv, recv, drecv, send):
    chan, bins = lax.axis_index("chan"), lax.axis_index("bins")
    zdim = lax.axis_size("chan") // ydim
    nbins = lax.axis_size("bins")
    z, y = chan // ydim, chan % ydim
    x, core = bins // 2, bins % 2
    held = parts_ref.shape[0] // nbins
    issued = []

    def device(zz, yy, xx, kk):
        return {"chan": zz * ydim + yy, "bins": xx * 2 + kk}

    def copy(src, dst, recv_sem, target, cond=None):
        made = pltpu.make_async_remote_copy(
            src_ref=src,
            dst_ref=dst,
            send_sem=send.at[len(issued)],
            recv_sem=recv_sem,
            device_id=target,
            device_id_type=pl.DeviceIdType.MESH,
        )
        issued.append((made, cond))
        run(cond, made.start)

    def run(cond, action):
        if cond is None:
            action()
        else:
            pl.when(cond)(action)

    partner = device(z, y, x, 1 - core)
    beside = device(z, y, 1 - x, core)
    below_there, above_there = z > 0, z < zdim - 1

    barrier = pltpu.get_barrier_semaphore()
    for target, cond in (
        (partner, None),
        (beside, None),
        (device(z, 1 - y, x, core), None),
        (device(z - 1, y, x, core), below_there),
        (device(z + 1, y, x, core), above_there),
    ):
        run(cond, lambda target=target: pl.semaphore_signal(
            barrier, 1, device_id=target, device_id_type=pl.DeviceIdType.MESH
        ))
    pl.semaphore_wait(barrier, 3 + jnp.minimum(z, 1) + jnp.minimum(zdim - 1 - z, 1))

    far, near = (1 - x) * 2, x * 2
    for half, owner in enumerate((far, near)):
        for i in range(held):
            copy(
                parts_ref.at[(owner + 1 - core) * held + i],
                swap.at[half * held + i],
                swap_recv.at[half * held + i],
                partner,
            )

    def arrived(dst, sem):
        pltpu.make_async_remote_copy(
            src_ref=dst, dst_ref=dst, send_sem=send.at[0], recv_sem=sem,
            device_id=partner, device_id_type=pl.DeviceIdType.MESH,
        ).wait_recv()

    for i in range(held):
        arrived(swap.at[i], swap_recv.at[i])
        total[i] = parts_ref[(far + core) * held + i] + swap[i]
        copy(total.at[i], cross.at[i], cross_recv.at[i], beside)
    base = bins * held + chan * nbins * held
    for i in range(held):
        arrived(swap.at[held + i], swap_recv.at[held + i])
        arrived(cross.at[i], cross_recv.at[i])
        out_ref[base + i] = (
            parts_ref[(near + core) * held + i] + swap[held + i]
        ) + cross[i]

    events = []
    for color, (_, _, order) in enumerate(COLORS):
        for dz in range(1 - zdim, zdim):
            for fx in range(2):
                for fy in range(2):
                    events.append((abs(dz) + fx + fy, fx + fy, color, dz, fx, fy))
    events.sort()
    for _, _, color, dz, fx, fy in events:
        first, count, order = COLORS[color]
        sz, sx, sy = z + dz, (1 - x if fx else x), (1 - y if fy else y)
        chip = (sz * ydim + sy) * 2 + sx
        there = None if dz == 0 else (z >= -dz if dz < 0 else z < zdim - dz)
        at = ((sz * ydim + sy) * nbins + sx * 2 + core) * held
        piece = out_ref.at[pl.ds(at, held), pl.ds(first, count)]
        offset = {"z": dz, "x": fx, "y": fy}
        last = max([n for n, d in enumerate(order) if offset[d]], default=-1)
        sem = recv.at[color, chip]
        if last >= 0:
            run(there, lambda piece=piece, sem=sem: arrived(piece, sem))

        def both(a, b):
            return b if a is None else (a if b is None else jnp.logical_and(a, b))

        if zdim > 1:
            onward = order.index("z") > last
            if (onward or (last >= 0 and order[last] == "z" and dz < 0)) and dz >= 2 - zdim:
                copy(piece, piece, sem, device(z + 1, y, x, core), both(there, above_there))
            if (onward or (last >= 0 and order[last] == "z" and dz > 0)) and dz <= zdim - 2:
                copy(piece, piece, sem, device(z - 1, y, x, core), both(there, below_there))
        if order.index("x") > last:
            copy(piece, piece, sem, beside, there)
        if order.index("y") > last:
            copy(piece, piece, sem, device(z, 1 - y, x, core), there)
        copy(piece, piece, drecv.at[color, chip], partner, there)

    for color, (first, count, _) in enumerate(COLORS):
        for chip in range(zdim * ydim * 2):
            at = (chip // 2 * nbins + chip % 2 * 2 + 1 - core) * held
            arrived(out_ref.at[pl.ds(at, held), pl.ds(first, count)], drecv.at[color, chip])
    for made, cond in issued:
        run(cond, made.wait_send)


def exchange(parts):
    nbins, nchan = lax.axis_size("bins"), lax.axis_size("chan")
    chans, rows, width = parts.shape
    held = chans // nbins
    whole = pl.BlockSpec(memory_space=pltpu.VMEM)
    chips = nchan * nbins // 2
    return pl.pallas_call(
        functools.partial(exchange_kernel, 2),
        in_specs=[whole],
        out_specs=whole,
        out_shape=jax.ShapeDtypeStruct((nchan * chans, rows, width), jnp.float32),
        scratch_shapes=[
            pltpu.VMEM((2 * held, rows, width), jnp.float32),
            pltpu.VMEM((held, rows, width), jnp.float32),
            pltpu.VMEM((held, rows, width), jnp.float32),
            pltpu.SemaphoreType.DMA((2 * held,)),
            pltpu.SemaphoreType.DMA((held,)),
            pltpu.SemaphoreType.DMA((len(COLORS), chips)),
            pltpu.SemaphoreType.DMA((len(COLORS), chips)),
            pltpu.SemaphoreType.DMA((SENDS,)),
        ],
        compiler_params=pltpu.CompilerParams(
            collective_id=0, has_side_effects=True, vmem_limit_bytes=32 * 2**20
        ),
        name="exchange",
    )(parts)


SENDS = 240


def local(effects, nominal, observed, mc_variance, theta, nuisance_index, bin_counts, tile_owner):
    devices = lax.axis_size("chan") * lax.axis_size("bins")
    device = lax.axis_index("chan") * lax.axis_size("bins") + lax.axis_index("bins")
    total_nu = theta.shape[0]
    slice_len = total_nu // devices
    groups = nuisance_index[:, ::GW] // GW
    parts = curvature(effects, nominal, observed, mc_variance, theta, groups, bin_counts)
    chan_size, bins_size = lax.axis_size("chan"), lax.axis_size("bins")
    if bins_size == 4 and chan_size % 2 == 0 and chan_size // 2 <= DEEP:
        payload = exchange(parts)
    else:
        summed = lax.psum_scatter(parts, "bins", scatter_dimension=0, tiled=True)
        payload = lax.all_gather(summed, ("chan", "bins"), axis=0, tiled=True)
    tiles, grad = place(
        payload, theta, groups, tile_owner, tile_owner.shape[0] // devices, max(1, slice_len // GW)
    )
    gradient = grad.reshape(-1)
    if slice_len < GW:
        gradient = lax.dynamic_slice_in_dim(gradient, device * slice_len % GW, slice_len, 0)
    return (tiles, gradient)


def solution(mesh):
    return jax.shard_map(
        local,
        mesh=mesh,
        in_specs=(
            P("chan", "bins", None),
            P("chan", "bins"),
            P("chan", "bins"),
            P("chan", "bins"),
            P(),
            P(),
            P("chan"),
            P(),
        ),
        out_specs=(P(("chan", "bins"), None, None), P(("chan", "bins"))),
        check_vma=False,
    )
```

```python
import functools

import jax
import jax.numpy as jnp
from jax import lax
from jax.experimental import pallas as pl
from jax.experimental.pallas import tpu as pltpu
from jax.sharding import PartitionSpec as P

GW = 128
TILE = 512
EXTRA = 8


def channel_payload(eff, chosen, nominal, observed, variance, live):
    eff_t = eff.T
    exponent = jnp.dot(chosen, eff_t, preferred_element_type=jnp.float32)[0:8]
    expected = nominal * jnp.exp(exponent)
    denominator = 1.0 + expected * variance
    residual = jnp.where(live, (expected - observed) / denominator, 0.0)
    weight = jnp.where(live, expected / denominator, 0.0)
    weighted = (eff_t.astype(jnp.float32) * weight[0:1]).astype(jnp.bfloat16)
    residual_rows = jnp.concatenate([residual, residual], axis=0).astype(jnp.bfloat16)
    left = jnp.concatenate([weighted, residual_rows], axis=0)
    full = jnp.dot(left, eff, preferred_element_type=jnp.float32)
    first, off, second = full[:GW, :GW], full[:GW, GW:], full[GW : 2 * GW, GW:]
    row = lax.broadcasted_iota(jnp.int32, (GW, GW), 0)
    col = lax.broadcasted_iota(jnp.int32, (GW, GW), 1)
    packed = jnp.where(row <= col, first, second)
    second_diag = jnp.sum(jnp.where(row == col, second, 0.0), axis=0, keepdims=True)
    grad0 = full[2 * GW : 2 * GW + 8, :GW]
    grad1 = full[2 * GW : 2 * GW + 8, GW:]
    which = lax.broadcasted_iota(jnp.int32, (EXTRA, GW), 0)
    extra = jnp.where(
        which == 0, grad0, jnp.where(which == 1, grad1, jnp.broadcast_to(second_diag, (EXTRA, GW)))
    )
    return packed, off, extra


def curvature_kernel(groups_ref, counts_ref, eff_ref, nom_ref, obs_ref, var_ref, theta_ref, out_ref):
    chan = lax.axis_index("chan")
    bins = lax.axis_index("bins")
    c = pl.program_id(0)
    size = eff_ref.shape[1]
    base = chan * pl.num_programs(0) + c
    g0, g1 = groups_ref[base, 0], groups_ref[base, 1]
    chosen = jnp.concatenate([theta_ref[g0], theta_ref[g1]], axis=1).astype(jnp.bfloat16)
    chosen = jnp.broadcast_to(chosen, (16, 2 * GW))
    line = pl.ds(c, 1)
    nominal, observed, variance = nom_ref[line], obs_ref[line].astype(jnp.float32), var_ref[line]
    position = bins * size + lax.broadcasted_iota(jnp.int32, (8, size), 1)
    packed, off, extra = channel_payload(
        eff_ref[0], chosen, nominal, observed, variance, position < counts_ref[c]
    )
    out_ref[0, :GW] = packed
    out_ref[0, GW : 2 * GW] = off
    out_ref[0, 2 * GW :] = extra


def curvature(effects, nominal, observed, variance, theta, groups, counts):
    chans, size, width = effects.shape
    rows = 2 * GW + EXTRA
    whole = lambda *shape: pl.BlockSpec(shape, lambda c, *_: (0,) * len(shape))
    return pl.pallas_call(
        curvature_kernel,
        grid_spec=pltpu.PrefetchScalarGridSpec(
            num_scalar_prefetch=2,
            grid=(chans,),
            in_specs=[
                pl.BlockSpec((1, size, width), lambda c, *_: (c, 0, 0)),
                whole(chans, size),
                whole(chans, size),
                whole(chans, size),
                whole(theta.shape[0] // GW, 1, GW),
            ],
            out_specs=pl.BlockSpec((1, rows, GW), lambda c, *_: (c, 0, 0)),
        ),
        out_shape=jax.ShapeDtypeStruct((chans, rows, GW), jnp.float32),
        compiler_params=pltpu.CompilerParams(vmem_limit_bytes=58 * 2**20),
        name="curvature",
    )(
        groups,
        counts,
        effects,
        nominal,
        observed,
        variance,
        theta.reshape(-1, 1, GW),
    )


def place_kernel(
    groups_ref, owner_ref, payload_ref, theta_ref, tiles_ref, grad_ref,
    lookup, entries, counts,
):
    step = pl.program_id(0)
    slots = counts.shape[0] - 1
    device = lax.axis_index("chan") * lax.axis_size("bins") + lax.axis_index("bins")
    chans = payload_ref.shape[0]
    per_tile = TILE // GW
    total_groups = theta_ref.shape[0]
    side = total_groups // per_tile
    shift = per_tile.bit_length() - 1
    room = 4 * chans
    start = device * slots

    @pl.when(step == 0)
    def _():
        def clear(i, _):
            for j in range(16):
                lookup[i * 16 + j] = slots
            return 0

        lax.fori_loop(0, side * side // 16, clear, 0)
        counts[slots] = 0
        for s in range(slots):
            counts[s] = 0
            lookup[owner_ref[start + s]] = s

        def visit(pair, _):
            for c in (pair * 2, pair * 2 + 1):
                a, b = groups_ref[c, 0], groups_ref[c, 1]
                ta, tb = a >> shift, b >> shift
                ra, rb = a & (per_tile - 1), b & (per_tile - 1)
                cases = ((ta, ta, ra, ra), (tb, tb, rb, rb), (ta, tb, ra, rb), (tb, ta, rb, ra))
                for kind, (tr, tc, rr, rc) in enumerate(cases):
                    slot = lookup[tr * side + tc]
                    n = counts[slot]
                    entries[slot * room + n] = ((((c << shift) + rr) << shift) + rc) * 4 + kind
                    counts[slot] = n + 1
            return 0

        lax.fori_loop(0, chans // 2, visit, 0)

    tile = owner_ref[start + step]

    tiles_ref[...] = jnp.zeros_like(tiles_ref)
    eye = (
        lax.broadcasted_iota(jnp.int32, (GW, GW), 0) == lax.broadcasted_iota(jnp.int32, (GW, GW), 1)
    ).astype(jnp.float32)

    @pl.when(tile // side == tile % side)
    def _():
        for r in range(per_tile):
            tiles_ref[0, r * GW : (r + 1) * GW, r * GW : (r + 1) * GW] = eye

    row = lax.broadcasted_iota(jnp.int32, (GW, GW), 0)
    col = lax.broadcasted_iota(jnp.int32, (GW, GW), 1)

    def accumulate(i, _):
        code = entries[step * room + i]
        kind = code & 3
        rc = (code >> 2) & (per_tile - 1)
        rr = (code >> (2 + shift)) & (per_tile - 1)
        c = code >> (2 + 2 * shift)
        at = (
            0,
            pl.ds(pl.multiple_of(rr * GW, GW), GW),
            pl.ds(pl.multiple_of(rc * GW, GW), GW),
        )

        @pl.when(kind == 0)
        def _():
            upper = jnp.where(row <= col, payload_ref[c, :GW], 0.0)
            tiles_ref[at] += upper + jnp.where(row > col, upper.T, 0.0)

        @pl.when(kind == 1)
        def _():
            lower = jnp.where(row > col, payload_ref[c, :GW], 0.0)
            diag = jnp.where(row == col, payload_ref[c, 2 * GW + 2 : 2 * GW + 3], 0.0)
            tiles_ref[at] += lower + lower.T + diag

        @pl.when(kind == 2)
        def _():
            tiles_ref[at] += payload_ref[c, GW : 2 * GW]

        @pl.when(kind == 3)
        def _():
            tiles_ref[at] += payload_ref[c, GW : 2 * GW].T

        return 0

    lax.fori_loop(0, counts[step], accumulate, 0)

    @pl.when(step == slots - 1)
    def _():
        mine = grad_ref.shape[0]
        first = device * total_groups // (lax.axis_size("chan") * lax.axis_size("bins"))
        for m in range(mine):
            grad_ref[m] = theta_ref[first + m]

        def add(c, _):
            for r in range(2):
                m = groups_ref[c, r] - first

                @pl.when(jnp.logical_and(m >= 0, m < mine))
                def _(m=m, r=r):
                    grad_ref[m] += payload_ref[c, 2 * GW + r : 2 * GW + r + 1]

            return 0

        lax.fori_loop(0, chans, add, 0)


def place(payload, theta, groups, tile_owner, slots, mine):
    chans, rows = payload.shape[:2]
    return pl.pallas_call(
        place_kernel,
        grid_spec=pltpu.PrefetchScalarGridSpec(
            num_scalar_prefetch=2,
            grid=(slots,),
            in_specs=[
                pl.BlockSpec(memory_space=pltpu.VMEM),
                pl.BlockSpec((theta.shape[0] // GW, 1, GW), lambda s, *_: (0, 0, 0)),
            ],
            out_specs=[
                pl.BlockSpec((1, TILE, TILE), lambda s, *_: (s, 0, 0)),
                pl.BlockSpec((mine, 1, GW), lambda s, *_: (0, 0, 0)),
            ],
            scratch_shapes=[
                pltpu.SMEM((tile_owner.shape[0],), jnp.int32),
                pltpu.SMEM(((slots + 1) * chans * 4,), jnp.int32),
                pltpu.SMEM((slots + 1,), jnp.int32),
            ],
        ),
        out_shape=[
            jax.ShapeDtypeStruct((slots, TILE, TILE), jnp.float32),
            jax.ShapeDtypeStruct((mine, 1, GW), jnp.float32),
        ],
        compiler_params=pltpu.CompilerParams(
            vmem_limit_bytes=4 * chans * (rows + EXTRA) * GW + 8 * 2**20
        ),
        name="place",
    )(groups, tile_owner, payload, theta.reshape(-1, 1, GW))


COLORS = ((0, 104, "zxy"), (104, 104, "zyx"), (208, 56, "xyz"))
DEEP = 4


def exchange_kernel(
    ydim, groups_ref, counts_ref, eff_ref, nom_ref, obs_ref, var_ref, theta_ref, out_ref,
    eff_held, parts_ref, swap, cross, total, eff_sem, swap_recv, cross_recv, recv, drecv, send,
):
    chan, bins = lax.axis_index("chan"), lax.axis_index("bins")
    zdim = lax.axis_size("chan") // ydim
    nbins = lax.axis_size("bins")
    z, y = chan // ydim, chan % ydim
    x, core = bins // 2, bins % 2
    held = parts_ref.shape[0] // nbins
    issued = []

    def device(zz, yy, xx, kk):
        return {"chan": zz * ydim + yy, "bins": xx * 2 + kk}

    def copy(src, dst, recv_sem, target, cond=None):
        made = pltpu.make_async_remote_copy(
            src_ref=src,
            dst_ref=dst,
            send_sem=send.at[len(issued)],
            recv_sem=recv_sem,
            device_id=target,
            device_id_type=pl.DeviceIdType.MESH,
        )
        issued.append((made, cond))
        run(cond, made.start)

    def run(cond, action):
        if cond is None:
            action()
        else:
            pl.when(cond)(action)

    partner = device(z, y, x, 1 - core)
    beside = device(z, y, 1 - x, core)
    below_there, above_there = z > 0, z < zdim - 1

    barrier = pltpu.get_barrier_semaphore()
    for target, cond in (
        (partner, None),
        (beside, None),
        (device(z, 1 - y, x, core), None),
        (device(z - 1, y, x, core), below_there),
        (device(z + 1, y, x, core), above_there),
    ):
        run(cond, lambda target=target: pl.semaphore_signal(
            barrier, 1, device_id=target, device_id_type=pl.DeviceIdType.MESH
        ))
    far, near = (1 - x) * 2, x * 2
    owners = (far + 1 - core, far + core, near + 1 - core, near + core)
    size = eff_ref.shape[1]

    def load(q, i):
        at = q * held + i
        return pltpu.make_async_copy(eff_ref.at[owners[q] * held + i], eff_held.at[at], eff_sem.at[at])

    for q in range(4):
        for i in range(held):
            load(q, i).start()

    def compute(q):
        for i in range(held):
            load(q, i).wait()

        def one(i, _):
            c = owners[q] * held + i
            base = chan * nbins * held + c
            g0, g1 = groups_ref[base, 0], groups_ref[base, 1]
            chosen = jnp.concatenate([theta_ref[g0], theta_ref[g1]], axis=1).astype(jnp.bfloat16)
            chosen = jnp.broadcast_to(chosen, (16, 2 * GW))
            line = pl.ds(c, 1)
            position = bins * size + lax.broadcasted_iota(jnp.int32, (8, size), 1)
            packed, off, extra = channel_payload(
                eff_held[q * held + i],
                chosen,
                nom_ref[line],
                obs_ref[line].astype(jnp.float32),
                var_ref[line],
                position < counts_ref[c],
            )
            parts_ref[q * held + i, :GW] = packed
            parts_ref[q * held + i, GW : 2 * GW] = off
            parts_ref[q * held + i, 2 * GW :] = extra
            return 0

        lax.fori_loop(0, held, one, 0)

    def arrived(dst, sem):
        pltpu.make_async_remote_copy(
            src_ref=dst, dst_ref=dst, send_sem=send.at[0], recv_sem=sem,
            device_id=partner, device_id_type=pl.DeviceIdType.MESH,
        ).wait_recv()

    def to_partner(q):
        for i in range(held):
            n = q // 2 * held + i
            copy(parts_ref.at[q * held + i], swap.at[n], swap_recv.at[n], partner)

    compute(0)
    pl.semaphore_wait(barrier, 3 + jnp.minimum(z, 1) + jnp.minimum(zdim - 1 - z, 1))
    to_partner(0)
    compute(1)
    for i in range(held):
        arrived(swap.at[i], swap_recv.at[i])
        total[i] = parts_ref[held + i] + swap[i]
        copy(total.at[i], cross.at[i], cross_recv.at[i], beside)
    compute(2)
    to_partner(2)
    compute(3)
    base = bins * held + chan * nbins * held
    for i in range(held):
        arrived(swap.at[held + i], swap_recv.at[held + i])
        arrived(cross.at[i], cross_recv.at[i])
        out_ref[base + i] = (parts_ref[3 * held + i] + swap[held + i]) + cross[i]

    events = []
    for color, (_, _, order) in enumerate(COLORS):
        for dz in range(1 - zdim, zdim):
            for fx in range(2):
                for fy in range(2):
                    events.append((abs(dz) + fx + fy, fx + fy, color, dz, fx, fy))
    events.sort()
    for _, _, color, dz, fx, fy in events:
        first, count, order = COLORS[color]
        sz, sx, sy = z + dz, (1 - x if fx else x), (1 - y if fy else y)
        chip = (sz * ydim + sy) * 2 + sx
        there = None if dz == 0 else (z >= -dz if dz < 0 else z < zdim - dz)
        at = ((sz * ydim + sy) * nbins + sx * 2 + core) * held
        piece = out_ref.at[pl.ds(at, held), pl.ds(first, count)]
        offset = {"z": dz, "x": fx, "y": fy}
        last = max([n for n, d in enumerate(order) if offset[d]], default=-1)
        sem = recv.at[color, chip]
        if last >= 0:
            run(there, lambda piece=piece, sem=sem: arrived(piece, sem))

        def both(a, b):
            return b if a is None else (a if b is None else jnp.logical_and(a, b))

        if zdim > 1:
            onward = order.index("z") > last
            if (onward or (last >= 0 and order[last] == "z" and dz < 0)) and dz >= 2 - zdim:
                copy(piece, piece, sem, device(z + 1, y, x, core), both(there, above_there))
            if (onward or (last >= 0 and order[last] == "z" and dz > 0)) and dz <= zdim - 2:
                copy(piece, piece, sem, device(z - 1, y, x, core), both(there, below_there))
        if order.index("x") > last:
            copy(piece, piece, sem, beside, there)
        if order.index("y") > last:
            copy(piece, piece, sem, device(z, 1 - y, x, core), there)
        copy(piece, piece, drecv.at[color, chip], partner, there)

    for color, (first, count, _) in enumerate(COLORS):
        for chip in range(zdim * ydim * 2):
            at = (chip // 2 * nbins + chip % 2 * 2 + 1 - core) * held
            arrived(out_ref.at[pl.ds(at, held), pl.ds(first, count)], drecv.at[color, chip])
    for made, cond in issued:
        run(cond, made.wait_send)


def exchange(effects, nominal, observed, variance, theta, groups, counts):
    nbins, nchan = lax.axis_size("bins"), lax.axis_size("chan")
    chans, size, channel_width = effects.shape
    rows, width = 2 * GW + EXTRA, GW
    held = chans // nbins
    vmem = pl.BlockSpec(memory_space=pltpu.VMEM)
    smem = pl.BlockSpec(memory_space=pltpu.SMEM)
    chips = nchan * nbins // 2
    return pl.pallas_call(
        functools.partial(exchange_kernel, 2),
        in_specs=[smem, smem, pl.BlockSpec(memory_space=pltpu.HBM), vmem, vmem, vmem, vmem],
        out_specs=vmem,
        out_shape=jax.ShapeDtypeStruct((nchan * chans, rows, width), jnp.float32),
        scratch_shapes=[
            pltpu.VMEM((chans, size, channel_width), jnp.bfloat16),
            pltpu.VMEM((chans, rows, width), jnp.float32),
            pltpu.VMEM((2 * held, rows, width), jnp.float32),
            pltpu.VMEM((held, rows, width), jnp.float32),
            pltpu.VMEM((held, rows, width), jnp.float32),
            pltpu.SemaphoreType.DMA((chans,)),
            pltpu.SemaphoreType.DMA((2 * held,)),
            pltpu.SemaphoreType.DMA((held,)),
            pltpu.SemaphoreType.DMA((len(COLORS), chips)),
            pltpu.SemaphoreType.DMA((len(COLORS), chips)),
            pltpu.SemaphoreType.DMA((SENDS,)),
        ],
        compiler_params=pltpu.CompilerParams(
            collective_id=0, has_side_effects=True, vmem_limit_bytes=32 * 2**20
        ),
        name="exchange",
    )(groups, counts, pltpu.with_memory_space_constraint(effects, pltpu.HBM), nominal, observed, variance, theta.reshape(-1, 1, GW))


SENDS = 240


def local(effects, nominal, observed, mc_variance, theta, nuisance_index, bin_counts, tile_owner):
    devices = lax.axis_size("chan") * lax.axis_size("bins")
    device = lax.axis_index("chan") * lax.axis_size("bins") + lax.axis_index("bins")
    total_nu = theta.shape[0]
    slice_len = total_nu // devices
    groups = nuisance_index[:, ::GW] // GW
    arrays = (effects, nominal, observed, mc_variance, theta, groups, bin_counts)
    chan_size, bins_size = lax.axis_size("chan"), lax.axis_size("bins")
    if bins_size == 4 and chan_size % 2 == 0 and chan_size // 2 <= DEEP:
        payload = exchange(*arrays)
    else:
        summed = lax.psum_scatter(curvature(*arrays), "bins", scatter_dimension=0, tiled=True)
        payload = lax.all_gather(summed, ("chan", "bins"), axis=0, tiled=True)
    tiles, grad = place(
        payload, theta, groups, tile_owner, tile_owner.shape[0] // devices, max(1, slice_len // GW)
    )
    gradient = grad.reshape(-1)
    if slice_len < GW:
        gradient = lax.dynamic_slice_in_dim(gradient, device * slice_len % GW, slice_len, 0)
    return (tiles, gradient)


def solution(mesh):
    return jax.shard_map(
        local,
        mesh=mesh,
        in_specs=(
            P("chan", "bins", None),
            P("chan", "bins"),
            P("chan", "bins"),
            P("chan", "bins"),
            P(),
            P(),
            P("chan"),
            P(),
        ),
        out_specs=(P(("chan", "bins"), None, None), P(("chan", "bins"))),
        check_vma=False,
    )
```
